32 devices in a mesh: rep: 8 (over z, y), shard: 4 (over x, core).
Axes of the slice: x: 2, y: 2, z: 4, core: 2. Of those that a mesh axis runs over, the one named last changes fastest.
Arguments:
- prompt: bfloat16 [8, 1024, 768], P('rep', 'shard'), may hold values from -6 to 6
- conts: bfloat16 [8, 4, 512, 768], P('rep', 'shard'), may hold values from -6 to 6
- prompt_cot: bfloat16 [8, 1024, 768], P('rep', 'shard'), may hold values from -6 to 6
- cont_cot: bfloat16 [8, 4, 512, 768], P('rep', 'shard'), may hold values from -6 to 6
- labels: int32 [8, 4], P('rep', 'shard'), may hold values from 0 to 13
- w_qkv: float32 [768, 2304], P('shard'), may hold values from -0.21875 to 0.21875
- w_out: float32 [768, 768], P('shard'), may hold values from -3.5 to 3.5
- w_in: float32 [768, 3072], P('shard'), may hold values from -0.21875 to 0.21875
- w_ffo: float32 [3072, 768], P('shard'), may hold values from -0.109375 to 0.109375
- layer_biases: float32 [6, 768], replicated, may hold values from -3 to 3
- norm_gains: float32 [2, 768], replicated, may hold values from 0.25 to 1.75
- bias_in: float32 [3072], replicated, may hold values from -3 to 3
- w_student: float32 [768, 128], replicated, may hold values from -0.21875 to 0.21875
- student_vectors: float32 [3, 128], replicated, may hold values from -4 to 4
- w_pool: float32 [128, 128], replicated, may hold values from -0.5 to 0.5
- w_class: float32 [128, 14], replicated, may hold values from -1 to 1
- bias_class: float32 [14], replicated, may hold values from -3 to 3
Outputs:
- prompt_out: bfloat16 [8, 1024, 768], P('rep', 'shard')
- cont_out: bfloat16 [8, 4, 512, 768], P('rep', 'shard')
- logits: float32 [8, 4, 14], P('rep', 'shard')
- prompt_grad: float32 [8, 1024, 768], P('rep', 'shard')
- cont_grad: float32 [8, 4, 512, 768], P('rep', 'shard')
- grad_qkv: float32 [768, 2304], P('shard')
- grad_out: float32 [768, 768], P('shard')
- grad_in: float32 [768, 3072], P('shard')
- grad_ffo: float32 [3072, 768], P('shard')
- grad_biases: float32 [6, 768], replicated
- grad_gains: float32 [2, 768], replicated
- grad_bias_in: float32 [3072], replicated
- grad_student: float32 [768, 128], replicated
- grad_student_vectors: float32 [3, 128], replicated
- grad_pool: float32 [128, 128], replicated
- grad_class: float32 [128, 14], replicated
- grad_bias_class: float32 [14], replicated
The draws below stay inside these ranges and needn't reach their ends.
All inputs are finite; a program needn't handle non-finite values.
Results may differ from the reference program's by a relative error of at most 0.02.
Values may be sent and summed in bfloat16 or wider, within the bound.
A program may use at most 192 MiB of HBM per device.

```python
from functools import partial
import jax
import jax.numpy as jnp
from jax import lax

D = 768
HEADS = 12
DH = 64
FF = 3072
STU = 128
SHEADS = 2
CLASSES = 14
PD = 256
CL = 512
PROMPT = 1024
GROUPS = 8
CONTS = 4


def place_ends(drawn, key, least, high):
    dims = drawn.shape
    index_at = [jax.random.randint(jax.random.fold_in(key, axis), (), 0, dims[axis]) for axis in range(len(dims))]
    drawn = drawn.at[tuple(index_at)].set(least)
    longest = dims.index(max(dims))
    index_at[longest] = (index_at[longest] + 1) % dims[longest]
    return drawn.at[tuple(index_at)].set(high)


def block_scale(own_key, shape, pieces, low, top_value):
    level, own = 1.0, jax.random.fold_in(own_key, 6)
    for dim, blocks in pieces:
        draws = jnp.exp(jax.random.uniform(jax.random.fold_in(own, dim), (blocks,), jnp.float32, low / len(pieces), top_value / len(pieces)))
        level = level * jnp.repeat(draws, shape[dim] // blocks).reshape([-1 if axis == dim else 1 for axis in range(len(shape))])
    return level


def gaussian(stream_key, dims, scale, limit, pieces=(), kind=jnp.bfloat16):
    drawn = jax.random.normal(stream_key, dims, jnp.float32) * scale
    if len(pieces) > 0:
        drawn = block_scale(stream_key, dims, pieces, -0.22, 0.18) * drawn
    return jnp.clip(drawn, min=-limit, max=limit).astype(kind)


def setup_inputs(seed: int = 0) -> dict:
    key_list = jax.random.split(jax.random.key(seed), 18)
    return {
        "prompt": gaussian(key_list[0], (GROUPS, PROMPT, D), 1.0, 6.0, ((0, 8), (1, 4))),
        "conts": gaussian(key_list[1], (GROUPS, CONTS, CL, D), 1.0, 6.0, ((0, 8), (1, 4))),
        "prompt_cot": gaussian(key_list[2], (GROUPS, PROMPT, D), 1.0, 6.0, ((0, 8), (1, 4))),
        "cont_cot": gaussian(key_list[3], (GROUPS, CONTS, CL, D), 1.0, 6.0, ((0, 8), (1, 4))),
        "labels": place_ends(jax.random.randint(key_list[4], (GROUPS, CONTS), 0, CLASSES), jax.random.fold_in(key_list[4], 1), 0, CLASSES - 1).astype(jnp.int32),
        "w_qkv": gaussian(key_list[5], (D, 3 * D), D ** -0.5, 0.21875, ((0, 4),), jnp.float32),
        "w_out": gaussian(key_list[6], (D, D), (max(D // 256, 1)) ** -0.5, 3.5, ((0, 4),), jnp.float32),
        "w_in": gaussian(key_list[7], (D, FF), D ** -0.5, 0.21875, ((0, 4),), jnp.float32),
        "w_ffo": gaussian(key_list[8], (FF, D), FF ** -0.5, 0.109375, ((0, 4),), jnp.float32),
        "layer_biases": gaussian(key_list[9], (6, D), 0.5, 3.0, (), jnp.float32),
        "norm_gains": jnp.clip(1.0 + 0.15 * jax.random.normal(key_list[10], (2, D), jnp.float32), 0.25, 1.75),
        "bias_in": gaussian(key_list[11], (FF,), 0.5, 3.0, (), jnp.float32),
        "w_student": gaussian(key_list[12], (D, STU), D ** -0.5, 0.21875, (), jnp.float32),
        "student_vectors": gaussian(key_list[13], (3, STU), 1.0, 4.0, (), jnp.float32),
        "w_pool": gaussian(key_list[14], (STU, STU), STU ** -0.5, 0.5, (), jnp.float32),
        "w_class": gaussian(key_list[15], (STU, CLASSES), (STU // 4) ** -0.5, 1.0, (), jnp.float32),
        "bias_class": gaussian(key_list[16], (CLASSES,), 0.5, 3.0, (), jnp.float32),
    }


@jax.custom_vjp
def low(v):
    return lax.optimization_barrier(v.astype(jnp.bfloat16)).astype(jnp.float32)

@jax.custom_vjp
def low_back(v):
    return v

def low_keep(v):
    return (low(v), None)

def low_pass(kept, grad):
    return (grad,)

def back_keep(v):
    return (v, None)

def back_low(kept, grad):
    return (low(grad),)
low.defvjp(low_keep, low_pass)
low_back.defvjp(back_keep, back_low)
HIGHEST = lax.Precision.HIGHEST
NEG_BIG = -1e+30

def matmul(left, right):
    return jnp.dot(left, right, precision=HIGHEST, preferred_element_type=jnp.float32)

def softmax_rows(scores):
    largest = lax.optimization_barrier(jnp.max(scores, -1, keepdims=True))
    expo = jnp.exp(scores - largest)
    return expo / lax.optimization_barrier(jnp.sum(expo, -1, keepdims=True))

def layer_norm(values, gain, shift):
    center = values - lax.optimization_barrier(jnp.mean(values, -1, keepdims=True))
    spread = lax.optimization_barrier(jnp.mean(center * center, -1, keepdims=True))
    return center * lax.rsqrt(spread + 1e-05) * gain + shift

def block_attention(kv_prompt, item):
    block_index, query_rows, kv_cont = item
    kv_seen = low_back(kv_prompt)
    keys = jnp.concatenate([kv_seen[:, :D], kv_cont[:, :D]], 0)
    values = jnp.concatenate([kv_seen[:, D:], kv_cont[:, D:]], 0)
    query_h = query_rows.reshape(-1, HEADS, DH)
    key_h = keys.reshape(-1, HEADS, DH)
    value_h = values.reshape(-1, HEADS, DH)
    scores = low_back(jnp.einsum('qhd,khd->hqk', query_h, key_h, precision=HIGHEST) * DH ** (-0.5))
    query_pos = jnp.concatenate([block_index * PD + jnp.arange(PD, dtype=jnp.int32), PROMPT + jnp.arange(CL, dtype=jnp.int32)])
    key_pos = jnp.arange(PROMPT + CL, dtype=jnp.int32)
    scores = jnp.where((key_pos[None, :] <= query_pos[:, None])[None], scores, NEG_BIG)
    attended = jnp.einsum('hqk,khd->qhd', low(softmax_rows(scores)), value_h, precision=HIGHEST)
    return attended.reshape(-1, D)

def student_head(stu_rows, pool_query, bias_pool, w_pool, w_class, bias_class):
    part_w = STU // SHEADS
    parts = stu_rows.reshape(CL, SHEADS, part_w)
    queries = pool_query.reshape(SHEADS, part_w)
    scores = jnp.einsum('tha,ha->ht', parts, queries, precision=HIGHEST) * part_w ** (-0.5)
    weights = softmax_rows(scores)
    pooled = jnp.einsum('ht,tha->ha', weights, parts, precision=HIGHEST).reshape(STU)
    top_layer = jnp.tanh(matmul(pooled, w_pool) + bias_pool)
    return matmul(top_layer, w_class) + bias_class

def group_forward(params, x_prompt, x_conts, cot_all, label_row):
    w_qkv, w_out, w_in, w_ffo, layer_biases, norm_gains, bias_in, w_student, student_vectors, w_pool, w_class, bias_class = params
    tokens = jnp.concatenate([x_prompt, x_conts.reshape(CONTS * CL, D)], 0)
    zero_row = jnp.zeros((D,), jnp.float32)
    bias_three = jnp.concatenate([layer_biases[0], zero_row, layer_biases[1]])
    qkv_raw = matmul(tokens, low(w_qkv)) + bias_three
    queries = low(low_back(qkv_raw[:, :D]))
    kv_prompt = low(qkv_raw[:PROMPT, D:])
    kv_cont = low(low_back(qkv_raw[PROMPT:, D:])).reshape(CONTS, CL, 2 * D)
    query_blocks = jnp.concatenate([queries[:PROMPT].reshape(CONTS, PD, D), queries[PROMPT:].reshape(CONTS, CL, D)], 1)
    blocks = lax.map(jax.checkpoint(partial(block_attention, kv_prompt)), (jnp.arange(CONTS, dtype=jnp.int32), query_blocks, kv_cont))
    attended_raw = jnp.concatenate([blocks[:, :PD].reshape(PROMPT, D), blocks[:, PD:].reshape(CONTS * CL, D)], 0)
    attended = low(low_back(attended_raw))
    branch = low_back(matmul(attended, low(w_out)) + layer_biases[2])
    first = layer_norm(tokens + branch, norm_gains[0], layer_biases[4])
    hidden = low_back(matmul(low(first), low(w_in)) + bias_in)
    ffn = low_back(matmul(low(jax.nn.gelu(hidden, approximate=False)), low(w_ffo)) + layer_biases[3])
    output = layer_norm(first + ffn, norm_gains[1], layer_biases[5])
    out_cont = output[PROMPT:].reshape(CONTS, CL, D)
    stu = low_back(jnp.einsum('cqd,de->cqe', low(out_cont), low(w_student), precision=HIGHEST) + student_vectors[0])
    logit_rows = jax.vmap(student_head, in_axes=(0, None, None, None, None, None))(stu, student_vectors[1], student_vectors[2], w_pool, w_class, bias_class)
    largest = lax.optimization_barrier(jnp.max(logit_rows, -1, keepdims=True))
    log_total = jnp.log(lax.optimization_barrier(jnp.sum(jnp.exp(logit_rows - largest), -1))) + largest[:, 0]
    picked = lax.optimization_barrier(jnp.sum(jnp.where(jnp.arange(CLASSES)[None, :] == label_row[:, None], logit_rows, 0.0), -1))
    objective = jnp.sum(output * cot_all) + jnp.sum(log_total - picked)
    return (objective, (output, logit_rows))

def reference(prompt, conts, prompt_cot, cont_cot, labels, w_qkv, w_out, w_in, w_ffo, layer_biases, norm_gains, bias_in, w_student, student_vectors, w_pool, w_class, bias_class):
    params = (w_qkv, w_out, w_in, w_ffo, layer_biases, norm_gains, bias_in, w_student, student_vectors, w_pool, w_class, bias_class)

    def group_step(totals, item):
        x_prompt, x_conts, cot_prompt, cot_conts, label_row = item
        cot_all = jnp.concatenate([cot_prompt.astype(jnp.float32), cot_conts.astype(jnp.float32).reshape(CONTS * CL, D)], 0)

        def closed(par, xp, xc):
            return group_forward(par, xp, xc, cot_all, label_row)
        objective, pull, extra = jax.vjp(closed, params, x_prompt.astype(jnp.float32), x_conts.astype(jnp.float32), has_aux=True)
        grad_par, grad_prompt, grad_conts = pull(jnp.ones((), jnp.float32))
        totals = jax.tree.map(jnp.add, totals, grad_par)
        output, logit_rows = extra
        outs = (output[:PROMPT].astype(jnp.bfloat16), output[PROMPT:].reshape(CONTS, CL, D).astype(jnp.bfloat16), logit_rows, grad_prompt, grad_conts)
        return (totals, outs)
    zeros = jax.tree.map(jnp.zeros_like, params)
    totals, ys = lax.scan(group_step, zeros, (prompt, conts, prompt_cot, cont_cot, labels))
    return (ys[0], ys[1], ys[2], ys[3], ys[4], totals[0], totals[1], totals[2], totals[3], totals[4], totals[5], totals[6], totals[7], totals[8], totals[9], totals[10], totals[11])
```

```python
from functools import partial

import jax
import jax.numpy as jnp
from jax import lax
from jax.experimental import pallas as pl
from jax.experimental.pallas import tpu as pltpu
from jax.sharding import PartitionSpec as P

D = 768
HEADS = 12
DH = 64
STU = 128
SHEADS = 2


HIGHEST = lax.Precision.HIGHEST
NEG_BIG = -1e30
ATTN_VMEM = 48 * 1024 * 1024


def dot_plain(left, right):
    return jnp.dot(left, right, preferred_element_type=jnp.float32)


def dot_first(left, right):
    return lax.dot_general(
        left, right, (((0,), (0,)), ((), ())), preferred_element_type=jnp.float32
    )


def dot_second(left, right):
    return lax.dot_general(
        left, right, (((1,), (1,)), ((), ())), preferred_element_type=jnp.float32
    )


def layer_norm(values, gain, shift):
    center = values - jnp.mean(values, -1, keepdims=True)
    spread = jnp.mean(center * center, -1, keepdims=True)
    return center * lax.rsqrt(spread + 1e-05) * gain + shift


def gelu_exact(values):
    return jax.nn.gelu(values, approximate=False)


def aug_parts(values):
    high = values.astype(jnp.bfloat16).astype(jnp.float32)
    rest = values - high
    mid = rest.astype(jnp.bfloat16).astype(jnp.float32)
    return (high, mid, rest - mid)


def attend_forward_kernel(prompt_rows, prompt_len, q_ref, kp_ref, vp_ref, k_ref, v_ref, o_ref, lse_ref):
    half = (q_ref.shape[0] - prompt_rows) // 2
    mid = prompt_rows + half
    start = lax.axis_index("shard") * prompt_rows
    width = 2 * DH
    chunk = min(512, prompt_len)
    outs = []
    logs = []
    for head in range(2):
        def lane_mask(rows):
            lane = lax.broadcasted_iota(jnp.int32, (rows, width), 1)
            return (lane >= DH) if head else (lane < DH)

        def attend(queries, segments):
            rows = queries.shape[0]
            scaled = jnp.where(lane_mask(rows), queries * jnp.bfloat16(DH ** (-0.5)), jnp.bfloat16(0))
            scores = []
            largest = None
            for keys, values, mask in segments:
                part = dot_second(scaled, keys)
                if mask is not None:
                    part = jnp.where(mask, part, NEG_BIG)
                scores.append(part)
                top = jnp.max(part, 1, keepdims=True)
                largest = top if largest is None else jnp.maximum(largest, top)
            total = None
            for part, (keys, values, mask) in zip(scores, segments):
                probs = jnp.exp(part - largest).astype(jnp.bfloat16)
                ones = jnp.ones(values.shape, jnp.bfloat16)
                both = dot_plain(probs, jnp.concatenate([values, ones], 1))
                total = both if total is None else total + both
            norm = total[:, width:]
            return (total[:, :width] / norm, largest + jnp.log(norm))

        def prompt_segments(masked):
            found = []
            for at in range(0, prompt_len, chunk):
                mask = None
                if masked:
                    query = lax.broadcasted_iota(jnp.int32, (prompt_rows, chunk), 0) + start
                    key = lax.broadcasted_iota(jnp.int32, (prompt_rows, chunk), 1) + at
                    mask = key <= query
                found.append((kp_ref[at : at + chunk, :], vp_ref[at : at + chunk, :], mask))
            return found

        def causal(size):
            return lax.broadcasted_iota(jnp.int32, (size, size), 1) <= lax.broadcasted_iota(
                jnp.int32, (size, size), 0
            )

        first = (k_ref[prompt_rows:mid, :], v_ref[prompt_rows:mid, :])
        second = (k_ref[mid:, :], v_ref[mid:, :])
        pieces = [
            attend(q_ref[:prompt_rows, :], prompt_segments(True)),
            attend(q_ref[prompt_rows:mid, :], prompt_segments(False) + [first + (causal(half),)]),
            attend(
                q_ref[mid:, :],
                prompt_segments(False) + [first + (None,), second + (causal(half),)],
            ),
        ]
        outs.append(jnp.concatenate([piece[0] for piece in pieces], 0))
        logs.append(jnp.concatenate([piece[1] for piece in pieces], 0))
    left = lax.broadcasted_iota(jnp.int32, outs[0].shape, 1) < DH
    o_ref[...] = jnp.where(left, outs[0], outs[1]).astype(o_ref.dtype)
    lse_ref[...] = jnp.where(left, logs[0], logs[1])


def attend_forward(qkv_b, kv_prompt):
    rows = qkv_b.shape[0]
    prompt_len = kv_prompt.shape[0]
    prompt_rows = prompt_len // lax.axis_size("shard")
    cont_len = rows - prompt_rows
    width = 2 * DH
    pairs = D // width
    return pl.pallas_call(
        partial(attend_forward_kernel, prompt_rows, prompt_len),
        grid=(pairs,),
        in_specs=[
            pl.BlockSpec((rows, width), lambda pair: (0, pair)),
            pl.BlockSpec((prompt_len, width), lambda pair: (0, pair)),
            pl.BlockSpec((prompt_len, width), lambda pair: (0, pairs + pair)),
            pl.BlockSpec((rows, width), lambda pair: (0, pairs + pair)),
            pl.BlockSpec((rows, width), lambda pair: (0, 2 * pairs + pair)),
        ],
        out_specs=[
            pl.BlockSpec((rows, width), lambda pair: (0, pair)),
            pl.BlockSpec((rows, width), lambda pair: (0, pair)),
        ],
        out_shape=[
            jax.ShapeDtypeStruct((rows, D), jnp.bfloat16),
            jax.ShapeDtypeStruct((rows, D), jnp.float32),
        ],
        compiler_params=pltpu.CompilerParams(vmem_limit_bytes=ATTN_VMEM),
        name="attend_forward",
    )(qkv_b, kv_prompt, kv_prompt, qkv_b, qkv_b)


def attend_backward_kernel(
    prompt_rows, prompt_len, q_ref, kp_ref, vp_ref, k_ref, v_ref, o_ref, go_ref, lse_ref,
    gq_ref, gkp_ref, gvp_ref, gkc_ref, gvc_ref, acc_ref
):
    rows = q_ref.shape[0]
    cont_len = rows - prompt_rows
    half = cont_len // 2
    mid = prompt_rows + half
    start = lax.axis_index("shard") * prompt_rows
    width = 2 * DH
    scaling = DH ** (-0.5)
    low = jnp.bfloat16
    prods = o_ref[...].astype(jnp.float32) * go_ref[...].astype(jnp.float32)
    lane = lax.broadcasted_iota(jnp.int32, (rows, width), 1)
    left = lane < DH
    augmented = []
    for head in range(2):
        own = jnp.logical_not(left) if head else left
        at = 0 if head else DH
        delta = jnp.sum(jnp.where(own, prods, 0.0), 1, keepdims=True)
        log_total = lse_ref[:, head * DH : head * DH + 1]

        def extend(values, shift):
            high, middle, rest = aug_parts(-shift)
            extra = jnp.where(
                lane == at, high, jnp.where(lane == at + 1, middle, jnp.where(lane == at + 2, rest, 0.0))
            ).astype(low)
            return jnp.where(own, values, extra)

        augmented.append(
            (extend(q_ref[...] * low(scaling), log_total), extend(go_ref[...], delta))
        )
    acc_ref[...] = jnp.zeros_like(acc_ref)

    def one_block(keys, values, spans):
        size = keys.shape[0]
        key_lane = lax.broadcasted_iota(jnp.int32, (size, width), 1)
        key_left = key_lane < DH
        grads_k = []
        grads_v = []
        for head in range(2):
            at = 0 if head else DH
            ones = jnp.logical_and(key_lane >= at, key_lane < at + 3)
            own = jnp.logical_not(key_left) if head else key_left

            def extend(block):
                return jnp.where(own, block, jnp.where(ones, low(1), low(0)))

            keys_x, values_x = extend(keys), extend(values)
            q_x, go_x = augmented[head]
            grad_k = None
            grad_v = None
            for lo, hi, mask in spans:
                scores = dot_second(keys_x, q_x[lo:hi])
                if mask is not None:
                    scores = jnp.where(mask, scores, NEG_BIG)
                probs = jnp.exp(scores)
                g_scores = (probs * dot_second(values_x, go_x[lo:hi])).astype(low)
                part_v = dot_plain(probs.astype(low), go_ref[lo:hi, :])
                part_k = dot_plain(g_scores, q_ref[lo:hi, :])
                grad_k = part_k if grad_k is None else grad_k + part_k
                grad_v = part_v if grad_v is None else grad_v + part_v
                acc_ref[head, lo:hi, :] += dot_first(g_scores, keys)
            grads_k.append(grad_k)
            grads_v.append(grad_v)
        return (
            jnp.where(key_left, grads_k[0], grads_k[1]) * scaling,
            jnp.where(key_left, grads_v[0], grads_v[1]),
        )

    chunk = prompt_rows

    def prompt_block(index, carry):
        at = pl.multiple_of(index * chunk, chunk)
        key = lax.broadcasted_iota(jnp.int32, (chunk, prompt_rows), 0) + at
        query = lax.broadcasted_iota(jnp.int32, (chunk, prompt_rows), 1) + start
        grad_k, grad_v = one_block(
            kp_ref[pl.ds(at, chunk), :],
            vp_ref[pl.ds(at, chunk), :],
            [(0, prompt_rows, key <= query), (prompt_rows, rows, None)],
        )
        gkp_ref[pl.ds(at, chunk), :] = grad_k.astype(low)
        gvp_ref[pl.ds(at, chunk), :] = grad_v.astype(low)
        return carry

    lax.fori_loop(0, prompt_len // chunk, prompt_block, 0)
    causal = lax.broadcasted_iota(jnp.int32, (half, half), 0) <= lax.broadcasted_iota(
        jnp.int32, (half, half), 1
    )
    grad_k, grad_v = one_block(
        k_ref[prompt_rows:mid, :], v_ref[prompt_rows:mid, :], [(prompt_rows, mid, causal), (mid, rows, None)]
    )
    gkc_ref[:half, :] = grad_k.astype(low)
    gvc_ref[:half, :] = grad_v.astype(low)
    grad_k, grad_v = one_block(k_ref[mid:, :], v_ref[mid:, :], [(mid, rows, causal)])
    gkc_ref[half:, :] = grad_k.astype(low)
    gvc_ref[half:, :] = grad_v.astype(low)
    gq_ref[...] = (jnp.where(left, acc_ref[0], acc_ref[1]) * scaling).astype(low)


def attend_backward(qkv_b, kv_prompt, att_b, grad_att, log_totals):
    rows = qkv_b.shape[0]
    prompt_len = kv_prompt.shape[0]
    prompt_rows = prompt_len // lax.axis_size("shard")
    cont_len = rows - prompt_rows
    width = 2 * DH
    pairs = D // width

    def column(count):
        return pl.BlockSpec((count, width), lambda pair: (0, pair))

    return pl.pallas_call(
        partial(attend_backward_kernel, prompt_rows, prompt_len),
        grid=(pairs,),
        in_specs=[
            column(rows),
            column(prompt_len),
            pl.BlockSpec((prompt_len, width), lambda pair: (0, pairs + pair)),
            pl.BlockSpec((rows, width), lambda pair: (0, pairs + pair)),
            pl.BlockSpec((rows, width), lambda pair: (0, 2 * pairs + pair)),
            column(rows),
            column(rows),
            column(rows),
        ],
        out_specs=[column(rows), column(prompt_len), column(prompt_len), column(cont_len), column(cont_len)],
        out_shape=[
            jax.ShapeDtypeStruct((rows, D), jnp.bfloat16),
            jax.ShapeDtypeStruct((prompt_len, D), jnp.bfloat16),
            jax.ShapeDtypeStruct((prompt_len, D), jnp.bfloat16),
            jax.ShapeDtypeStruct((cont_len, D), jnp.bfloat16),
            jax.ShapeDtypeStruct((cont_len, D), jnp.bfloat16),
        ],
        scratch_shapes=[pltpu.VMEM((2, rows, width), jnp.float32)],
        compiler_params=pltpu.CompilerParams(vmem_limit_bytes=ATTN_VMEM),
        name="attend_backward",
    )(qkv_b, kv_prompt, kv_prompt, qkv_b, qkv_b, att_b, grad_att, log_totals)


def student_loss(stu_rows, pool_query, bias_pool, w_pool, w_class, bias_class, label_value):
    part_w = STU // SHEADS
    parts = stu_rows.reshape(stu_rows.shape[0], SHEADS, part_w)
    queries = pool_query.reshape(SHEADS, part_w)
    scores = jnp.einsum("tha,ha->ht", parts, queries, precision=HIGHEST) * part_w ** (-0.5)
    largest = jnp.max(scores, -1, keepdims=True)
    expo = jnp.exp(scores - largest)
    weights = expo / jnp.sum(expo, -1, keepdims=True)
    pooled = jnp.einsum("ht,tha->ha", weights, parts, precision=HIGHEST).reshape(STU)
    top_layer = jnp.tanh(jnp.dot(pooled, w_pool, precision=HIGHEST) + bias_pool)
    logit_row = jnp.dot(top_layer, w_class, precision=HIGHEST) + bias_class
    top_logit = jnp.max(logit_row)
    log_total = jnp.log(jnp.sum(jnp.exp(logit_row - top_logit))) + top_logit
    picked = jnp.sum(jnp.where(jnp.arange(logit_row.shape[0]) == label_value, logit_row, 0.0))
    return (log_total - picked, logit_row)


def body(
    prompt,
    conts,
    prompt_cot,
    cont_cot,
    labels,
    w_qkv,
    w_out,
    w_in,
    w_ffo,
    layer_biases,
    norm_gains,
    bias_in,
    w_student,
    student_vectors,
    w_pool,
    w_class,
    bias_class,
):
    prompt_rows = prompt.shape[1]
    qkv_low = w_qkv.astype(jnp.bfloat16)
    out_low = w_out.astype(jnp.bfloat16)
    in_low = w_in.astype(jnp.bfloat16)
    ffo_low = w_ffo.astype(jnp.bfloat16)
    qkv_full, out_full, in_full, ffo_full = (
        lax.all_gather(qkv_low, "shard", axis=0, tiled=True),
        lax.all_gather(out_low, "shard", axis=0, tiled=True),
        lax.all_gather(in_low, "shard", axis=0, tiled=True),
        lax.all_gather(ffo_low, "shard", axis=0, tiled=True),
    )
    tokens = jnp.concatenate([prompt[0], conts[0, 0]], 0)
    tokens_f = tokens.astype(jnp.float32)
    zero_row = jnp.zeros((D,), jnp.float32)
    bias_three = jnp.concatenate([layer_biases[0], zero_row, layer_biases[1]])
    qkv_b = (dot_plain(tokens, qkv_full) + bias_three).astype(jnp.bfloat16)
    kv_prompt = lax.all_gather(qkv_b[:prompt_rows, D:], "shard", axis=0, tiled=True)
    att_b, log_totals = attend_forward(qkv_b, kv_prompt)
    branch = dot_plain(att_b, out_full) + layer_biases[2]
    resid_one = tokens_f + branch
    first = layer_norm(resid_one, norm_gains[0], layer_biases[4])
    first_b = first.astype(jnp.bfloat16)
    hidden = dot_plain(first_b, in_full) + bias_in
    act_b = gelu_exact(hidden).astype(jnp.bfloat16)
    ffn = dot_plain(act_b, ffo_full) + layer_biases[3]
    resid_two = first + ffn
    output = layer_norm(resid_two, norm_gains[1], layer_biases[5])
    output_b = output.astype(jnp.bfloat16)
    cont_b = output_b[prompt_rows:]
    student_low = w_student.astype(jnp.bfloat16)
    stu = dot_plain(cont_b, student_low) + student_vectors[0]

    def loss_closed(stu_rows, pool_query, bias_pool, pool_weight, class_weight, class_bias):
        return student_loss(
            stu_rows, pool_query, bias_pool, pool_weight, class_weight, class_bias, labels[0, 0]
        )

    loss_value, loss_pull, logit_row = jax.vjp(
        loss_closed,
        stu,
        student_vectors[1],
        student_vectors[2],
        w_pool,
        w_class,
        bias_class,
        has_aux=True,
    )
    g_stu, g_query, g_pbias, g_pool, g_class, g_cbias = loss_pull(jnp.ones((), jnp.float32))
    g_stu_b = g_stu.astype(jnp.bfloat16)
    g_sbias = jnp.sum(g_stu_b.astype(jnp.float32), 0)
    g_student = dot_first(cont_b, g_stu_b)
    student_back = dot_second(g_stu_b, student_low)
    g_output = jnp.concatenate([prompt_cot[0], cont_cot[0, 0]], 0).astype(jnp.float32)
    g_output = g_output + jnp.concatenate(
        [jnp.zeros((prompt_rows, D), jnp.float32), student_back], 0
    )
    qkv_back, out_back, in_back, ffo_back = (
        lax.all_gather(qkv_low, "shard", axis=0, tiled=True),
        lax.all_gather(out_low, "shard", axis=0, tiled=True),
        lax.all_gather(in_low, "shard", axis=0, tiled=True),
        lax.all_gather(ffo_low, "shard", axis=0, tiled=True),
    )
    norm_two, norm_two_pull = jax.vjp(layer_norm, resid_two, norm_gains[1], layer_biases[5])
    g_resid_two, g_gain_two, g_shift_two = norm_two_pull(g_output)
    g_ffn_b = g_resid_two.astype(jnp.bfloat16)
    g_ffo = dot_first(act_b, g_ffn_b)
    g_ffo_bias = jnp.sum(g_ffn_b.astype(jnp.float32), 0)
    g_act = dot_second(g_ffn_b, ffo_back)
    gelu_value, gelu_pull = jax.vjp(gelu_exact, hidden)
    g_hidden_b = gelu_pull(g_act)[0].astype(jnp.bfloat16)
    g_in = dot_first(first_b, g_hidden_b)
    g_in_bias = jnp.sum(g_hidden_b.astype(jnp.float32), 0)
    g_first = g_resid_two + dot_second(g_hidden_b, in_back)
    norm_one, norm_one_pull = jax.vjp(layer_norm, resid_one, norm_gains[0], layer_biases[4])
    g_resid_one, g_gain_one, g_shift_one = norm_one_pull(g_first)
    g_branch_b = g_resid_one.astype(jnp.bfloat16)
    g_outw = dot_first(att_b, g_branch_b)
    g_out_bias = jnp.sum(g_branch_b.astype(jnp.float32), 0)
    g_att_b = dot_second(g_branch_b, out_back).astype(jnp.bfloat16)
    query_grad_b, g_kp, g_vp, g_kc, g_vc = attend_backward(
        qkv_b, kv_prompt, att_b, g_att_b, log_totals
    )
    cont_kv_b = jnp.concatenate([g_kc, g_vc], 1)
    block_kv_b = jnp.concatenate([g_kp, g_vp], 1)
    kv_weights = qkv_back[:, D:]
    g_query_w = dot_first(tokens, query_grad_b)
    g_kv_w = dot_first(tokens[prompt_rows:], cont_kv_b)
    g_tokens = g_resid_one + dot_second(query_grad_b, qkv_back[:, :D])
    cont_through = dot_second(cont_kv_b, kv_weights)
    kv_summed = lax.psum_scatter(
        block_kv_b,
        "shard",
        scatter_dimension=0,
        tiled=True,
    ).astype(jnp.float32)
    g_kv_w = g_kv_w + lax.dot_general(
        tokens_f[:prompt_rows],
        kv_summed,
        (((0,), (0,)), ((), ())),
        precision=HIGHEST,
        preferred_element_type=jnp.float32,
    )
    prompt_through = jnp.dot(
        kv_summed,
        kv_weights.astype(jnp.float32).T,
        precision=HIGHEST,
        preferred_element_type=jnp.float32,
    )
    value_cols = jnp.sum(kv_summed[:, D:], 0)
    g_tokens = g_tokens + jnp.concatenate([prompt_through, cont_through], 0)
    g_qkvw = jnp.concatenate([g_query_w, g_kv_w], 1)
    g_query_bias = jnp.sum(query_grad_b.astype(jnp.float32), 0)
    g_value_bias = jnp.sum(cont_kv_b[:, D:].astype(jnp.float32), 0) + value_cols
    owned = (
        lax.psum_scatter(
            g_qkvw.astype(jnp.bfloat16), "shard", scatter_dimension=0, tiled=True
        ).astype(jnp.float32),
        lax.psum_scatter(
            g_outw.astype(jnp.bfloat16), "shard", scatter_dimension=0, tiled=True
        ).astype(jnp.float32),
        lax.psum_scatter(
            g_in.astype(jnp.bfloat16), "shard", scatter_dimension=0, tiled=True
        ).astype(jnp.float32),
        lax.psum_scatter(
            g_ffo.astype(jnp.bfloat16), "shard", scatter_dimension=0, tiled=True
        ).astype(jnp.float32),
    )
    owned_qkv, owned_out, owned_in, owned_ffo = (
        lax.psum(owned[0].astype(jnp.bfloat16), "rep").astype(jnp.float32),
        lax.psum(owned[1].astype(jnp.bfloat16), "rep").astype(jnp.float32),
        lax.psum(owned[2].astype(jnp.bfloat16), "rep").astype(jnp.float32),
        lax.psum(owned[3].astype(jnp.bfloat16), "rep").astype(jnp.float32),
    )
    g_biases = jnp.stack(
        [g_query_bias, g_value_bias, g_out_bias, g_ffo_bias, g_shift_one, g_shift_two]
    )
    g_gains = jnp.stack([g_gain_one, g_gain_two])
    g_vectors = jnp.stack([g_sbias, g_query, g_pbias])
    summed = lax.psum(
        (g_biases, g_gains, g_in_bias, g_student, g_vectors, g_pool, g_class, g_cbias),
        ("rep", "shard"),
    )
    return (
        output_b[:prompt_rows][None],
        output_b[prompt_rows:][None, None],
        logit_row[None, None],
        g_tokens[:prompt_rows][None],
        g_tokens[prompt_rows:][None, None],
        owned_qkv,
        owned_out,
        owned_in,
        owned_ffo,
        summed[0],
        summed[1],
        summed[2],
        summed[3],
        summed[4],
        summed[5],
        summed[6],
        summed[7],
    )


def solution(mesh):
    return jax.shard_map(
        body,
        mesh=mesh,
        in_specs=(
            P("rep", "shard", None),
            P("rep", "shard", None, None),
            P("rep", "shard", None),
            P("rep", "shard", None, None),
            P("rep", "shard"),
            P("shard", None),
            P("shard", None),
            P("shard", None),
            P("shard", None),
            P(),
            P(),
            P(),
            P(),
            P(),
            P(),
            P(),
            P(),
        ),
        out_specs=(
            P("rep", "shard", None),
            P("rep", "shard", None, None),
            P("rep", "shard", None),
            P("rep", "shard", None),
            P("rep", "shard", None, None),
            P("shard", None),
            P("shard", None),
            P("shard", None),
            P("shard", None),
            P(),
            P(),
            P(),
            P(),
            P(),
            P(),
            P(),
            P(),
        ),
        check_vma=False,
    )
```
